32 devices in a mesh: tm: 2 (over x), space: 16 (over z, y, core).
Axes of the slice: x: 2, y: 2, z: 4, core: 2. Of those that a mesh axis runs over, the one named last changes fastest.
Arguments:
- slice_ends: float32 [8, 2, 64, 16, 256], P('tm', None, 'space'), may hold values from 0.05 to 0.6
- initial: float32 [2, 64, 16, 256], P(None, 'space'), may hold values from 0.05 to 0.6
- feed_rate: float32 [64, 16, 256], P('space'), may hold values from 0.02 to 0.12
- kill_rate: float32 [64, 16, 256], P('space'), may hold values from 0.03 to 0.12
Outputs:
- new_ends: float32 [8, 2, 64, 16, 256], P('tm', None, 'space')
The draws below stay inside these ranges and needn't reach their ends.
All inputs are finite; a program needn't handle non-finite values.
Results may differ from the reference program's by a relative error of at most 0.0001.
Values sent between devices are 32-bit elements; how exact they have to be, the bound alone decides.
No kernel may reach another device: no remote copies, remote signals or barrier semaphores. Data moves between devices by JAX's collectives and lax.ppermute only.
A program may use at most 64 MiB of HBM per device.

```python
import math
import jax
import jax.numpy as jnp
from jax import lax

CY = 16
CZ = 256
NF = 8
KC = 8
SLICES = 8
NX = 64


def wave_states(key, count):
    keys = jax.random.split(key, 5)
    position = jnp.arange(NX).astype(jnp.float32) / NX
    phases = jax.random.uniform(keys[0], (count, 2, 1), jnp.float32, 0.0, 6.2831853)
    heights = jax.random.uniform(keys[1], (count, 2, 1), jnp.float32, 0.08, 0.16)
    modes = jax.random.randint(keys[2], (count, 2, 1), 1, 3).astype(jnp.float32)
    profile = heights * jnp.sin(6.2831853 * modes * position[None, None, :] + phases)
    noise = jnp.clip(0.03 * jax.random.normal(keys[4], (count, 2, NX, CY, CZ), jnp.float32), -0.08, 0.08)
    middle = 0.32 + jnp.zeros((count, 2, 1), jnp.float32)
    values = (middle + profile)[:, :, :, None, None] + noise
    return jnp.clip(values, 0.05, 0.6).astype(jnp.float32)


def draw_slice_ends(key, part):
    return wave_states(jax.random.fold_in(key, 11), SLICES)


def draw_initial(key, part):
    return wave_states(jax.random.fold_in(key, 23), 1)[0]


def level_of(rng, dims, shards, least, high):
    def one(axis_at, parts):
        steps = jax.random.uniform(jax.random.fold_in(jax.random.fold_in(rng, 6), axis_at), (parts,), jnp.float32, least / len(shards), high / len(shards))
        return jnp.repeat(jnp.exp(steps), dims[axis_at] // parts).reshape((-1,) + (1,) * (len(dims) - axis_at - 1))

    loudness = one(*shards[0])
    for cut in shards[1:]:
        loudness = loudness * one(*cut)
    return loudness


def setup_inputs(seed: int = 0) -> dict:
    seeds = jax.random.split(jax.random.key(seed), 5)
    return {
        "slice_ends": draw_slice_ends(jax.random.fold_in(seeds[4], 71), 0),
        "initial": draw_initial(jax.random.fold_in(seeds[4], 71), 0),
        "feed_rate": jnp.clip(jnp.exp(math.log(0.12) - 1.7917595 * jax.random.uniform(seeds[2], (NX, CY, CZ), jnp.float32) ** level_of(seeds[2], (NX, CY, CZ), ((0, 16),), -0.2, 0.2)), 0.02, 0.12),
        "kill_rate": jnp.clip(jnp.exp(math.log(0.12) - 1.3862944 * jax.random.uniform(seeds[3], (NX, CY, CZ), jnp.float32) ** level_of(seeds[3], (NX, CY, CZ), ((0, 16),), -0.2, 0.2)), 0.03, 0.12),
    }


spread_fast = 0.14
spread_slow = 0.07
fine_step = 0.25
coarse_step = 1.0


def neighbours(values):
    along_x = jnp.roll(values, 1, -3) + jnp.roll(values, -1, -3)
    along_y = jnp.roll(values, 1, -2) + jnp.roll(values, -1, -2)
    along_z = jnp.roll(values, 1, -1) + jnp.roll(values, -1, -1)
    return along_x + along_y + along_z - 6.0 * values


def advance(fields, feed_values, kill_values, time_step):
    substrate = fields[0]
    catalyst = fields[1]
    reaction = substrate * catalyst * catalyst
    new_sub = substrate + spread_fast * neighbours(substrate) + time_step * (feed_values * (1.0 - substrate) - reaction)
    new_cat = catalyst + spread_slow * neighbours(catalyst) + time_step * (reaction - (feed_values + kill_values) * catalyst)
    return jnp.stack([new_sub, new_cat])


def propagate(fields, feed_values, kill_values, time_step, repeats):
    for outer_step in range(repeats):
        fields = advance(fields, feed_values, kill_values, time_step)
    return fields


def restrict(values):
    leading = values.shape[:-3]
    sizes_x, sizes_y, sizes_z = values.shape[-3:]
    blocks = values.reshape(leading + (sizes_x // 2, 2, sizes_y // 2, 2, sizes_z // 2, 2))
    return jnp.mean(blocks, axis=(-5, -3, -1))


def prolong(values):
    return jnp.repeat(jnp.repeat(jnp.repeat(values, 2, -3), 2, -2), 2, -1)


def reference(slice_ends, initial, feed_rate, kill_rate):
    starts = jnp.concatenate([initial[None], slice_ends[:-1]], axis=0)

    def fine_slice(fields):
        return propagate(fields, feed_rate, kill_rate, fine_step, NF)

    fine_ends = lax.map(fine_slice, starts)
    coarse_feed = restrict(feed_rate)
    coarse_kill = restrict(kill_rate)

    def coarse(fields):
        return propagate(fields, coarse_feed, coarse_kill, coarse_step, KC)

    quartets = SLICES // 4
    offset = jnp.zeros((2, NX // 2, CY // 2, CZ // 2), jnp.float32)
    collected = [offset]
    for turn_index in range(quartets - 1):
        coarse_point = 4 * turn_index + 3
        coarse_guess = restrict(fine_ends[coarse_point]) + offset
        offset = coarse(coarse_guess) - coarse(restrict(slice_ends[coarse_point]))
        collected.append(offset)
    stacked = prolong(jnp.stack(collected))
    grouped = fine_ends.reshape(quartets, 4, 2, NX, CY, CZ) + stacked[:, None]
    return grouped.reshape(SLICES, 2, NX, CY, CZ)
```

```python
import jax
import jax.numpy as jnp
import numpy as np
from jax import lax
from jax.experimental import pallas as pl
from jax.experimental.pallas import tpu as pltpu
from jax.sharding import PartitionSpec as P

NF = 8
KC = 8

spread_fast = 0.14
spread_slow = 0.07
fine_step = 0.25
coarse_step = 1.0

LANES = 128
CHUNKS = ((3,), (2, 1), (0,))

VMEM = pl.BlockSpec(memory_space=pltpu.VMEM)
SMEM = pl.BlockSpec(memory_space=pltpu.SMEM)


def head_block(shape):
    return pl.BlockSpec((1,) + tuple(shape[1:]), lambda i: (0,) * len(shape))


def whole_block(shape):
    return pl.BlockSpec(tuple(shape), lambda i: (0,) * len(shape))


def step_plane(read, coeffs, row):
    h_feed = coeffs(0, row)
    h_loss = coeffs(1, row)
    height, width = h_feed.shape
    out = []
    planes = [read(0, row), read(1, row)]
    sums = []
    for field in (0, 1):
        center = planes[field]
        total = read(field, row + 1) + read(field, row - 1)
        total = total + (pltpu.roll(center, 1, 0) + pltpu.roll(center, height - 1, 0))
        total = total + (pltpu.roll(center, 1, 1) + pltpu.roll(center, width - 1, 1))
        sums.append(total)
    return planes, sums, h_feed, h_loss


def advance_plane(read, coeffs, row, time_step):
    (substrate, catalyst), (sum_u, sum_v), h_feed, h_loss = step_plane(read, coeffs, row)
    reaction = (time_step * substrate) * (catalyst * catalyst)
    new_u = (1.0 - 6.0 * spread_fast) * substrate + spread_fast * sum_u + (h_feed * (1.0 - substrate) - reaction)
    new_v = (1.0 - 6.0 * spread_slow) * catalyst + spread_slow * sum_v + (reaction - h_loss * catalyst)
    return new_u, new_v


def pool_matrix(width):
    matrix = np.zeros((width, width // 2), np.float32)
    matrix[np.arange(width), np.arange(width) // 2] = 1.0
    return matrix


def restrict_planes(load, n_fields, rows, scratch, pool):
    halves = []
    for field in range(n_fields):
        for pair in range(rows // 2):
            slot = field * (rows // 2) + pair
            plane = load(field, 2 * pair) + load(field, 2 * pair + 1)
            half = plane.shape[0] // 2
            lanes = []
            for at in range(plane.shape[1] // LANES):
                spot = slot * (plane.shape[1] // LANES) + at
                scratch[spot] = plane[:, at * LANES : (at + 1) * LANES]
                lanes.append(scratch[spot, pl.ds(0, half, 2), :] + scratch[spot, pl.ds(1, half, 2), :])
            halves.append(jnp.concatenate(lanes, axis=1))
    stacked = jnp.concatenate(halves, axis=0)
    pooled = jnp.dot(stacked, pool, precision=lax.Precision.HIGHEST, preferred_element_type=jnp.float32)
    return pooled * 0.125


def fine_kernel(n, rows, steps, with_coarse):
    def kernel(parity, *refs):
        refs = list(refs)
        own_c, inn_c, out_c, own, inn, out = refs[:6]
        refs = refs[6:]
        pool = refs.pop(0) if with_coarse else None
        result = refs.pop(0)
        coarse_out = refs.pop(0) if with_coarse else None
        coef, ping, pong = refs[:3]
        scratch = refs[3] if with_coarse else None
        odd = parity[0]

        def gather_coef(low, high):
            feed = jnp.concatenate([low[0, 0], own_c[0, 0], high[0, 0]], axis=0)
            kill = jnp.concatenate([low[0, 1], own_c[0, 1], high[0, 1]], axis=0)
            coef[0] = fine_step * feed
            coef[1] = fine_step * (feed + kill)

        @pl.when(odd == 0)
        def _():
            gather_coef(out_c, inn_c)

        @pl.when(odd == 1)
        def _():
            gather_coef(inn_c, out_c)

        shift = own.shape[0] - n

        def one_slice(index, carry):
            source = index + shift
            ping[:, rows : 2 * rows] = own[source]

            @pl.when(odd == 0)
            def _():
                ping[:, 0:rows] = out[source]
                ping[:, 2 * rows : 3 * rows] = inn[source]

            @pl.when(odd == 1)
            def _():
                ping[:, 0:rows] = inn[source]
                ping[:, 2 * rows : 3 * rows] = out[source]

            buffers = (ping, pong)
            for step in range(steps):
                src, dst = buffers[step % 2], buffers[(step + 1) % 2]
                first = rows - steps + 1 + step
                last = 3 * rows - first
                for row in range(first, last):
                    new_u, new_v = advance_plane(
                        lambda field, r: src[field, r], lambda which, r: coef[which, r], row, fine_step
                    )
                    if step == steps - 1:
                        result[index, 0, row - rows] = new_u
                        result[index, 1, row - rows] = new_v
                    else:
                        dst[0, row] = new_u
                        dst[1, row] = new_v
            return carry

        lax.fori_loop(0, n, one_slice, 0)
        if with_coarse:
            pooled = restrict_planes(lambda f, r: result[0, f, r], 2, rows, scratch, pool[...])
            coarse_out[...] = pooled.reshape(coarse_out.shape)

    return kernel


def fine_call(parity, coeff_parts, parts, n, steps, with_coarse):
    rows, sy, sz = parts[0].shape[-3:]
    state = (n, 2, rows, sy, sz)
    operands = [parity, *coeff_parts, *parts]
    in_specs = [SMEM] + [head_block(c.shape) for c in coeff_parts] + [whole_block(p.shape) for p in parts]
    out_shape = [jax.ShapeDtypeStruct(state, jnp.float32)]
    out_specs = [whole_block(state)]
    scratch = [
        pltpu.VMEM((2, 3 * rows, sy, sz), jnp.float32),
        pltpu.VMEM((2, 3 * rows, sy, sz), jnp.float32),
        pltpu.VMEM((2, 3 * rows, sy, sz), jnp.float32),
    ]
    if with_coarse:
        pool = jnp.asarray(pool_matrix(sz))
        operands.append(pool)
        in_specs.append(whole_block(pool.shape))
        coarse = (2, rows // 2, sy // 2, sz // 2)
        out_shape.append(jax.ShapeDtypeStruct(coarse, jnp.float32))
        out_specs.append(whole_block(coarse))
        scratch.append(pltpu.VMEM((rows * sz // LANES, sy, LANES), jnp.float32))
    return pl.pallas_call(
        fine_kernel(n, rows, steps, with_coarse),
        grid=(1,),
        in_specs=in_specs,
        out_specs=out_specs,
        out_shape=out_shape,
        scratch_shapes=scratch,
        name="fine",
    )(*operands)


def early_kernel(feed, kill, last, pool, result, scratch):
    rows = feed.shape[0]

    def load(field, row):
        return (last[0, 0, row], last[0, 1, row], feed[row], kill[row])[field]

    pooled = restrict_planes(load, 4, rows, scratch, pool[...])
    result[...] = pooled.reshape(result.shape)


def early_call(slice_ends, feed_rate, kill_rate):
    count = slice_ends.shape[0]
    rows, sy, sz = feed_rate.shape
    pool = jnp.asarray(pool_matrix(sz))
    last = pl.BlockSpec((1,) + slice_ends.shape[1:], lambda i: (count - 1, 0, 0, 0, 0))
    shape = (4, rows // 2, sy // 2, sz // 2)
    return pl.pallas_call(
        early_kernel,
        grid=(1,),
        in_specs=[whole_block(feed_rate.shape), whole_block(kill_rate.shape), last, whole_block(pool.shape)],
        out_specs=whole_block(shape),
        out_shape=jax.ShapeDtypeStruct(shape, jnp.float32),
        scratch_shapes=[pltpu.VMEM((2 * rows * sz // LANES, sy, LANES), jnp.float32)],
        name="early",
    )(feed_rate, kill_rate, slice_ends, pool)


def coarse_solve(targets, launches, coef, ping, pong, rows):
    blocks = len(targets)
    total = blocks * rows
    for b in range(blocks):
        for r in range(rows):
            feed = coarse_step * launches[b][2, r]
            coef[0, b * rows + r] = feed
            coef[1, b * rows + r] = feed + coarse_step * launches[b][3, r]
            for field in (0, 1):
                ping[0, field, b * rows + r] = targets[b][field, r]
                ping[1, field, b * rows + r] = launches[b][field, r]
    middle = (blocks // 2) * rows
    buffers = (ping, pong)
    ends = []
    for step in range(KC):
        src, dst = buffers[step % 2], buffers[(step + 1) % 2]
        reach = KC - 1 - step
        for state in (0, 1):
            for row in range(middle - reach, middle + rows + reach):
                new_u, new_v = advance_plane(
                    lambda field, r: src[state, field, r], lambda which, r: coef[which, r], row, coarse_step
                )
                dst[state, 0, row] = new_u
                dst[state, 1, row] = new_v
    final = buffers[KC % 2]
    return [final[0, f, middle + r] - final[1, f, middle + r] for f in (0, 1) for r in range(rows)]


def coarse_kernel(blocks):
    def kernel(place, *refs):
        targets, launches = refs[:blocks], refs[blocks : 2 * blocks]
        result, coef, ping, pong = refs[2 * blocks :]
        rows = result.shape[1]
        keep = jnp.where(place[1] > 0, 1.0, 0.0)
        planes = coarse_solve(targets, launches, coef, ping, pong, rows)
        for i, plane in enumerate(planes):
            result[i // rows, i % rows] = plane * keep

    return kernel


def coarse_scratch(blocks, block):
    _, rows, sy, sz = block
    return [
        pltpu.VMEM((2, blocks * rows, sy, sz), jnp.float32),
        pltpu.VMEM((2, 2, blocks * rows, sy, sz), jnp.float32),
        pltpu.VMEM((2, 2, blocks * rows, sy, sz), jnp.float32),
    ]


def coarse_call(place, targets, launches):
    blocks = len(targets)
    shape = targets[0].shape
    return pl.pallas_call(
        coarse_kernel(blocks),
        grid=(1,),
        in_specs=[SMEM] + [whole_block(b.shape) for b in (*targets, *launches)],
        out_specs=whole_block(shape),
        out_shape=jax.ShapeDtypeStruct(shape, jnp.float32),
        scratch_shapes=coarse_scratch(blocks, shape),
        name="coarse",
    )(place, *targets, *launches)


def final_kernel(blocks, chunks):
    def kernel(place, *refs):
        targets, launches = refs[:blocks], refs[blocks : 2 * blocks]
        refs = refs[2 * blocks :]
        fines, spread = refs[: len(chunks)], refs[len(chunks)]
        result, coef, ping, pong, wide = refs[len(chunks) + 1 :]
        rows = targets[0].shape[1]
        keep = jnp.where(place[1] > 0, 1.0, 0.0)
        planes = coarse_solve(targets, launches, coef, ping, pong, rows)
        height = planes[0].shape[0]
        stacked = jnp.concatenate(planes, axis=0) * keep
        spread_out = jnp.dot(
            stacked, spread[...], precision=lax.Precision.HIGHEST, preferred_element_type=jnp.float32
        )
        for i in range(len(planes)):
            part = spread_out[i * height : (i + 1) * height]
            tiles = part.shape[1] // LANES
            for at in range(tiles):
                piece = part[:, at * LANES : (at + 1) * LANES]
                wide[i * tiles + at, pl.ds(0, height, 2), :] = piece
                wide[i * tiles + at, pl.ds(1, height, 2), :] = piece
            field, row = i // rows, i % rows
            plane = jnp.concatenate([wide[i * tiles + at] for at in range(tiles)], axis=1)
            for chunk, fine in zip(chunks, fines):
                for at, which in enumerate(chunk):
                    for half in (0, 1):
                        result[which, field, 2 * row + half] = fine[at, field, 2 * row + half] + plane

    return kernel


def final_call(place, targets, launches, fines, chunks, out_shape):
    blocks = len(targets)
    block = targets[0].shape
    sz = out_shape[-1]
    spread = jnp.asarray(pool_matrix(sz).T.copy())
    return pl.pallas_call(
        final_kernel(blocks, chunks),
        grid=(1,),
        in_specs=[SMEM]
        + [whole_block(b.shape) for b in (*targets, *launches, *fines)]
        + [whole_block(spread.shape)],
        out_specs=whole_block(out_shape),
        out_shape=jax.ShapeDtypeStruct(out_shape, jnp.float32),
        scratch_shapes=coarse_scratch(blocks, block)
        + [pltpu.VMEM((2 * block[1] * sz // LANES, out_shape[-2], LANES), jnp.float32)],
        name="final",
    )(place, *targets, *launches, *fines, spread)


def local(slice_ends, initial, feed_rate, kill_rate):
    rows = feed_rate.shape[0]
    count = slice_ends.shape[0]
    quartets = lax.axis_size("tm")
    size = lax.axis_size("space")
    tm = lax.axis_index("tm")
    space = lax.axis_index("space")
    parity = (space % 2).astype(jnp.int32).reshape(1)
    place = jnp.stack([space, tm]).astype(jnp.int32)
    inner_pairs = [(i, i ^ 1) for i in range(size)]
    outer_pairs = [(i, (i + 1) % size if i % 2 else (i - 1) % size) for i in range(size)]

    def exchange(value):
        outer = lax.ppermute(value, "space", outer_pairs)
        inner = lax.ppermute(value, "space", inner_pairs)
        return value, inner, outer

    reach = -(-KC // (rows // 2))

    def to_next(value, distance):
        pairs = []
        for t in range(quartets - 1):
            for s in range(size):
                pairs.append((t * size + (s + distance) % size, (t + 1) * size + s))
        return lax.ppermute(value, ("tm", "space"), pairs)

    distances = range(-reach, reach + 1)
    width = min(rows, NF)

    coeffs = jnp.stack([feed_rate, kill_rate])[None]
    first_own = jnp.concatenate([coeffs] + [slice_ends[i - 1 : i] for i in CHUNKS[0]], axis=0)
    first = exchange(first_own)

    shifted = to_next(slice_ends[count - 1 : count], 0)
    start = jnp.where(tm == 0, initial[None], shifted)

    owns = [first_own]
    exchanged = [first]
    for chunk in CHUNKS[1:]:
        own = jnp.concatenate([start if i == 0 else slice_ends[i - 1 : i] for i in chunk], axis=0)
        owns.append(own)
        exchanged.append(exchange(own))

    early = early_call(slice_ends, feed_rate, kill_rate)
    launches = [to_next(early, d) for d in distances]

    rounds = NF // width
    fines = [None] * len(CHUNKS)
    target = None
    parts = exchanged
    for turn in range(rounds):
        following = []
        for at, chunk in enumerate(CHUNKS):
            with_coarse = turn == rounds - 1 and at == 0
            got = fine_call(parity, first, parts[at], len(chunk), width, with_coarse)
            fines[at] = got[0]
            if with_coarse:
                target = got[1]
            if turn < rounds - 1:
                following.append(exchange(got[0]))
        parts = following

    offset = jnp.zeros_like(target)
    for turn in range(quartets - 2):
        sent = target + offset
        offset = coarse_call(place, [to_next(sent, d) for d in distances], launches)
    sent = target if quartets <= 2 else target + offset
    targets = [to_next(sent, d) for d in distances]
    return final_call(place, targets, launches, fines, CHUNKS, slice_ends.shape)


def solution(mesh):
    in_specs = (
        P("tm", None, "space", None, None),
        P(None, "space", None, None),
        P("space", None, None),
        P("space", None, None),
    )
    out_specs = P("tm", None, "space", None, None)
    return jax.shard_map(local, mesh=mesh, in_specs=in_specs, out_specs=out_specs, check_vma=False)
```

```python
import jax
import jax.numpy as jnp
import numpy as np
from jax import lax
from jax.experimental import pallas as pl
from jax.experimental.pallas import tpu as pltpu
from jax.sharding import PartitionSpec as P

NF = 8
KC = 8

spread_fast = 0.14
spread_slow = 0.07
fine_step = 0.25
coarse_step = 1.0

LANES = 128
FIRST = ((3,), (2, 1), (0,))
SECOND = ((3,), (2, 1, 0))

VMEM = pl.BlockSpec(memory_space=pltpu.VMEM)
SMEM = pl.BlockSpec(memory_space=pltpu.SMEM)


def near(value):
    return pltpu.with_memory_space_constraint(value, pltpu.VMEM)


def call(kernel, scalars, arrays, outs, scratch, far_out=False):
    shapes = [jax.ShapeDtypeStruct(o, jnp.float32) if far_out else pltpu.VMEM(o, jnp.float32) for o in outs]
    got = pl.pallas_call(
        kernel,
        in_specs=[SMEM] * len(scalars) + [VMEM] * len(arrays),
        out_specs=[VMEM] * len(outs),
        out_shape=shapes,
        scratch_shapes=[pltpu.VMEM(shape, jnp.float32) for shape in scratch],
    )(*scalars, *[near(a) for a in arrays])
    return got


def step_plane(read, coeffs, row):
    h_feed = coeffs(0, row)
    h_loss = coeffs(1, row)
    height, width = h_feed.shape
    planes = [read(0, row), read(1, row)]
    sums = []
    for field in (0, 1):
        center = planes[field]
        total = read(field, row + 1) + read(field, row - 1)
        total = total + (pltpu.roll(center, 1, 0) + pltpu.roll(center, height - 1, 0))
        total = total + (pltpu.roll(center, 1, 1) + pltpu.roll(center, width - 1, 1))
        sums.append(total)
    return planes, sums, h_feed, h_loss


def advance_plane(read, coeffs, row, time_step):
    (substrate, catalyst), (sum_u, sum_v), h_feed, h_loss = step_plane(read, coeffs, row)
    reaction = (time_step * substrate) * (catalyst * catalyst)
    new_u = (1.0 - 6.0 * spread_fast) * substrate + spread_fast * sum_u + (h_feed * (1.0 - substrate) - reaction)
    new_v = (1.0 - 6.0 * spread_slow) * catalyst + spread_slow * sum_v + (reaction - h_loss * catalyst)
    return new_u, new_v


def pool_matrix(width):
    matrix = np.zeros((width, width // 2), np.float32)
    matrix[np.arange(width), np.arange(width) // 2] = 1.0
    return matrix


def restrict_planes(load, n_fields, rows, scratch, pool):
    halves = []
    for field in range(n_fields):
        for pair in range(rows // 2):
            slot = field * (rows // 2) + pair
            plane = load(field, 2 * pair) + load(field, 2 * pair + 1)
            half = plane.shape[0] // 2
            lanes = []
            for at in range(plane.shape[1] // LANES):
                spot = slot * (plane.shape[1] // LANES) + at
                scratch[spot] = plane[:, at * LANES : (at + 1) * LANES]
                lanes.append(scratch[spot, pl.ds(0, half, 2), :] + scratch[spot, pl.ds(1, half, 2), :])
            halves.append(jnp.concatenate(lanes, axis=1))
    stacked = jnp.concatenate(halves, axis=0)
    pooled = jnp.dot(stacked, pool, precision=lax.Precision.HIGHEST, preferred_element_type=jnp.float32)
    return pooled * 0.125


def fine_kernel(plan, rows, steps, n_buffers, with_coarse):
    def kernel(parity, *refs):
        refs = list(refs)
        own_c, inn_c, out_c = [refs.pop(0) for _ in range(3)]
        buffers = [tuple(refs.pop(0) for _ in range(3)) for _ in range(n_buffers)]
        pool = refs.pop(0) if with_coarse else None
        result = refs.pop(0)
        coarse_out = refs.pop(0) if with_coarse else None
        coef, ping, pong = refs[:3]
        scratch = refs[3] if with_coarse else None
        odd = parity[0]

        def place_coef(source, at):
            for row in range(rows):
                feed = fine_step * source[0, 0, row]
                coef[0, at + row] = feed
                coef[1, at + row] = feed + fine_step * source[0, 1, row]

        def place_halos(index, source, low, high):
            ping[index, :, 0:rows] = low[source]
            ping[index, :, 2 * rows : 3 * rows] = high[source]

        place_coef(own_c, rows)
        for index, (at, source) in enumerate(plan):
            ping[index, :, rows : 2 * rows] = buffers[at][0][source]

        @pl.when(odd == 0)
        def _():
            place_coef(out_c, 0)
            place_coef(inn_c, 2 * rows)
            for index, (at, source) in enumerate(plan):
                place_halos(index, source, buffers[at][2], buffers[at][1])

        @pl.when(odd == 1)
        def _():
            place_coef(inn_c, 0)
            place_coef(out_c, 2 * rows)
            for index, (at, source) in enumerate(plan):
                place_halos(index, source, buffers[at][1], buffers[at][2])

        def one_slice(index, carry):
            pair = (ping, pong)
            for step in range(steps):
                src, dst = pair[step % 2], pair[(step + 1) % 2]
                first = rows - steps + 1 + step
                last = 3 * rows - first
                for row in range(first, last):
                    new_u, new_v = advance_plane(
                        lambda field, r: src[index, field, r], lambda which, r: coef[which, r], row, fine_step
                    )
                    if step == steps - 1:
                        result[index, 0, row - rows] = new_u
                        result[index, 1, row - rows] = new_v
                    else:
                        dst[index, 0, row] = new_u
                        dst[index, 1, row] = new_v
            return carry

        lax.fori_loop(0, len(plan), one_slice, 0)
        if with_coarse:
            pooled = restrict_planes(lambda f, r: result[0, f, r], 2, rows, scratch, pool[...])
            coarse_out[...] = pooled.reshape(coarse_out.shape)

    return kernel


def fine_call(parity, coeff_parts, buffers, plan, steps, with_coarse):
    rows, sy, sz = coeff_parts[0].shape[-3:]
    n = len(plan)
    arrays = [*coeff_parts] + [part for buffer in buffers for part in buffer]
    outs = [(n, 2, rows, sy, sz)]
    scratch = [(2, 3 * rows, sy, sz), (n, 2, 3 * rows, sy, sz), (n, 2, 3 * rows, sy, sz)]
    if with_coarse:
        arrays.append(jnp.asarray(pool_matrix(sz)))
        outs.append((2, rows // 2, sy // 2, sz // 2))
        scratch.append((rows * sz // LANES, sy, LANES))
    kernel = fine_kernel(tuple(plan), rows, steps, len(buffers), with_coarse)
    return call(kernel, [parity], arrays, outs, scratch)


def early_kernel(feed, kill, last, pool, result, scratch):
    rows = feed.shape[0]

    def load(field, row):
        return (last[0, 0, row], last[0, 1, row], feed[row], kill[row])[field]

    pooled = restrict_planes(load, 4, rows, scratch, pool[...])
    result[...] = pooled.reshape(result.shape)


def early_call(last, feed_rate, kill_rate):
    rows, sy, sz = feed_rate.shape
    pool = jnp.asarray(pool_matrix(sz))
    shape = (4, rows // 2, sy // 2, sz // 2)
    return call(early_kernel, [], [feed_rate, kill_rate, last, pool], [shape], [(2 * rows * sz // LANES, sy, LANES)])[0]


def spread_blocks(odd, fars, mine, theirs, put):
    depth = len(mine)

    @pl.when(odd == 0)
    def _():
        for at in range(depth):
            put(at, mine[at])
            put(2 * depth - at, theirs[at])

    @pl.when(odd == 1)
    def _():
        for at in range(depth):
            put(at, theirs[at])
            put(2 * depth - at, mine[at])

    put(depth, fars)


def march(ping, pong, coef, base, middle, rows):
    pair = (ping, pong)
    for step in range(KC):
        src, dst = pair[step % 2], pair[(step + 1) % 2]
        reach = KC - 1 - step
        for row in range(middle - reach, middle + rows + reach):
            new_u, new_v = advance_plane(
                lambda field, r: src[field, base + r], lambda which, r: coef[which, base + r], row, coarse_step
            )
            dst[0, base + row] = new_u
            dst[1, base + row] = new_v
    return pair[KC % 2]


def launch_kernel(depth, rows):
    def kernel(place, *refs):
        center, mine, theirs = refs[0], refs[1 : 1 + depth], refs[1 + depth : 1 + 2 * depth]
        result, coef, ping, pong = refs[1 + 2 * depth :]
        per = center.shape[1]

        def put(at, block):
            for r in range(per):
                row = at * per + r
                feed = coarse_step * block[2, r]
                coef[0, row] = feed
                coef[1, row] = feed + coarse_step * block[3, r]
                ping[0, row] = block[0, r]
                ping[1, row] = block[1, r]

        odd = place[0]
        spread_blocks(odd, center, mine, theirs, put)
        base = rows * odd
        final = march(ping, pong, coef, base, depth * per, rows)
        for field in (0, 1):
            for r in range(rows):
                result[field, r] = final[field, base + depth * per + r]

    return kernel


def launch_call(place, center, mine, theirs, rows):
    depth = len(mine)
    _, per, sy, sz = center.shape
    total = (2, (2 * depth + 1) * per, sy, sz)
    return call(
        launch_kernel(depth, rows), [place], [center, *mine, *theirs], [(2, rows, sy, sz), total], [total, total]
    )


def solve_planes(place, center, mine, theirs, launch, coef, ping, pong):
    depth, per, rows = len(mine), center.shape[1], launch.shape[1]

    def put(at, block):
        for r in range(per):
            ping[0, at * per + r] = block[0, r]
            ping[1, at * per + r] = block[1, r]

    odd = place[0]
    spread_blocks(odd, center, mine, theirs, put)
    base = rows * odd
    final = march(ping, pong, coef, base, depth * per, rows)
    keep = jnp.where(place[1] > 0, 1.0, 0.0)
    return [(final[f, base + depth * per + r] - launch[f, r]) * keep for f in (0, 1) for r in range(rows)]


def coarse_kernel(depth):
    def kernel(place, *refs):
        center, mine, theirs = refs[0], refs[1 : 1 + depth], refs[1 + depth : 1 + 2 * depth]
        launch, coef, result, ping, pong = refs[1 + 2 * depth :]
        rows = launch.shape[1]
        for i, plane in enumerate(solve_planes(place, center, mine, theirs, launch, coef, ping, pong)):
            result[i // rows, i % rows] = plane

    return kernel


def coarse_call(place, blocks, launch, coef):
    center, mine, theirs = blocks
    return call(
        coarse_kernel(len(mine)), [place], [center, *mine, *theirs, launch, coef], [launch.shape], [coef.shape, coef.shape]
    )[0]


def final_kernel(depth, chunks):
    def kernel(place, *refs):
        center, mine, theirs = refs[0], refs[1 : 1 + depth], refs[1 + depth : 1 + 2 * depth]
        refs = refs[1 + 2 * depth :]
        launch, coef = refs[:2]
        fines, spread = refs[2 : 2 + len(chunks)], refs[2 + len(chunks)]
        result, ping, pong, wide = refs[3 + len(chunks) :]
        rows = launch.shape[1]
        planes = solve_planes(place, center, mine, theirs, launch, coef, ping, pong)
        height = planes[0].shape[0]
        stacked = jnp.concatenate(planes, axis=0)
        spread_out = jnp.dot(
            stacked, spread[...], precision=lax.Precision.HIGHEST, preferred_element_type=jnp.float32
        )
        for i in range(len(planes)):
            part = spread_out[i * height : (i + 1) * height]
            tiles = part.shape[1] // LANES
            for at in range(tiles):
                piece = part[:, at * LANES : (at + 1) * LANES]
                wide[i * tiles + at, pl.ds(0, height, 2), :] = piece
                wide[i * tiles + at, pl.ds(1, height, 2), :] = piece
            field, row = i // rows, i % rows
            plane = jnp.concatenate([wide[i * tiles + at] for at in range(tiles)], axis=1)
            for chunk, fine in zip(chunks, fines):
                for at, which in enumerate(chunk):
                    for half in (0, 1):
                        result[which, field, 2 * row + half] = fine[at, field, 2 * row + half] + plane

    return kernel


def final_call(place, blocks, launch, coef, fines, chunks, out_shape):
    center, mine, theirs = blocks
    sz = out_shape[-1]
    spread = jnp.asarray(pool_matrix(sz).T.copy())
    return call(
        final_kernel(len(mine), chunks),
        [place],
        [center, *mine, *theirs, launch, coef, *fines, spread],
        [out_shape],
        [coef.shape, coef.shape, (2 * launch.shape[1] * sz // LANES, out_shape[-2], LANES)],
        far_out=True,
    )[0]


def whole_program(slice_ends, initial, feed_rate, kill_rate):
    rows = feed_rate.shape[0]
    count = slice_ends.shape[0]
    quartets = lax.axis_size("tm")
    size = lax.axis_size("space")
    tm = lax.axis_index("tm")
    odd = lax.axis_index("space") % 2
    place = jnp.stack([odd, tm]).astype(jnp.int32)
    inner_pairs = [(i, i ^ 1) for i in range(size)]
    outer_pairs = [(i, (i + 1) % size if i % 2 else (i - 1) % size) for i in range(size)]

    def swap(value):
        return lax.ppermute(value, "space", inner_pairs)

    def exchange(value):
        outer = lax.ppermute(value, "space", outer_pairs)
        return value, swap(value), outer

    def to_next(value, source):
        pairs = []
        for t in range(quartets):
            for s in range(size):
                pairs.append((t * size + source(s) % size, ((t + 1) % quartets) * size + s))
        return lax.ppermute(value, ("tm", "space"), pairs)

    coarse_rows = rows // 2
    depth = -(-KC // (2 * coarse_rows))

    def collect(value):
        other = swap(value)
        block = jnp.where(
            odd == 0, jnp.concatenate([value, other], axis=1), jnp.concatenate([other, value], axis=1)
        )
        mine = []
        for at in range(depth):
            reach = 2 * (depth - at)
            mine.append(to_next(block, lambda s: s + (reach if s % 2 else -reach)))
        center = to_next(block, lambda s: s)
        theirs = [swap(part) for part in mine]
        return center, mine, theirs

    width = min(rows, NF)
    assert width == rows and NF % width == 0 and size % 2 == 0
    rounds = NF // width

    coeffs = jnp.stack([feed_rate, kill_rate])[None]
    first_own = jnp.concatenate([coeffs] + [slice_ends[i - 1 : i] for i in FIRST[0]], axis=0)
    coef_parts = exchange(first_own)
    last = slice_ends[count - 1 : count]
    sent = jnp.where(tm == quartets - 1, initial[None], last)
    start = to_next(sent, lambda s: s)

    buffers = [coef_parts]
    for chunk in FIRST[1:]:
        own = jnp.concatenate([start if i == 0 else slice_ends[i - 1 : i] for i in chunk], axis=0)
        buffers.append(exchange(own))
    where = {i: (c, k + (1 if c == 0 else 0)) for c, chunk in enumerate(FIRST) for k, i in enumerate(chunk)}

    early = early_call(last, feed_rate, kill_rate)
    launch, coef = launch_call(place, *collect(early), coarse_rows)

    target = None
    for turn in range(rounds):
        fines, following = [], []
        for at, chunk in enumerate(SECOND):
            with_coarse = turn == rounds - 1 and at == 0
            used = sorted({where[i][0] for i in chunk})
            plan = [(used.index(where[i][0]), where[i][1]) for i in chunk]
            got = fine_call(place, coef_parts, [buffers[u] for u in used], plan, width, with_coarse)
            fines.append(got[0])
            if with_coarse:
                target = got[1]
            if turn < rounds - 1:
                following.append(exchange(got[0]))
        buffers = following
        where = {i: (c, k) for c, chunk in enumerate(SECOND) for k, i in enumerate(chunk)}

    sent = target
    for _ in range(quartets - 2):
        offset = coarse_call(place, collect(sent), launch, coef)
        sent = target + offset
    return final_call(place, collect(sent), launch, coef, fines, SECOND, slice_ends.shape)


def solution(mesh):
    in_specs = (
        P("tm", None, "space", None, None),
        P(None, "space", None, None),
        P("space", None, None),
        P("space", None, None),
    )
    out_specs = P("tm", None, "space", None, None)
    return jax.shard_map(whole_program, mesh=mesh, in_specs=in_specs, out_specs=out_specs, check_vma=False)
```

```python
import jax
import jax.numpy as jnp
from jax import lax
from jax.experimental import pallas as pl
from jax.experimental.pallas import tpu as pltpu
from jax.sharding import PartitionSpec as P


NF = 8
KC = 8

spread_fast = 0.14
spread_slow = 0.07
fine_step = 0.25
coarse_step = 1.0

LANES = 128
SUBLANES = 8
VMEM_LIMIT = 12 << 20
CHUNKS = ((3,), (2, 1), (0,))

VMEM = pl.BlockSpec(memory_space=pltpu.VMEM)
SMEM = pl.BlockSpec(memory_space=pltpu.SMEM)
ANY = pl.BlockSpec(memory_space=pl.ANY)
HBM = pl.BlockSpec(memory_space=pltpu.HBM)


def near(value):
    return pltpu.with_memory_space_constraint(value, pltpu.VMEM)


def far(value):
    return pltpu.with_memory_space_constraint(value, pltpu.HBM)


def call(kernel, scalars, arrays, outs, scratch, far_out=False):
    shapes = [jax.ShapeDtypeStruct(o, jnp.float32) if far_out else pltpu.VMEM(o, jnp.float32) for o in outs]
    got = pl.pallas_call(
        kernel,
        in_specs=[SMEM] * len(scalars) + [VMEM] * len(arrays),
        out_specs=[VMEM] * len(outs),
        out_shape=shapes,
        scratch_shapes=[pltpu.VMEM(shape, jnp.float32) for shape in scratch],
        compiler_params=pltpu.CompilerParams(vmem_limit_bytes=VMEM_LIMIT),
    )(*scalars, *[near(a) for a in arrays])
    return got


def store_coeffs(coef, row, feed, kill, time_step):
    h_feed = time_step * feed
    coef[0, row] = h_feed
    coef[1, row] = (1.0 - 6.0 * spread_fast) - h_feed
    coef[2, row] = (1.0 - 6.0 * spread_slow) - (h_feed + time_step * kill)


def padded_shape(lead, sy, sz):
    return (*lead, sz // LANES, sy + 2 * SUBLANES, LANES)


def put_plane(ref, at, plane):
    height = plane.shape[0]
    for tile in range(plane.shape[1] // LANES):
        part = plane[:, tile * LANES : (tile + 1) * LANES]
        ref[(*at, tile, slice(SUBLANES, SUBLANES + height))] = part
        ref[(*at, tile, slice(SUBLANES - 1, SUBLANES))] = part[height - 1 :]
        ref[(*at, tile, slice(SUBLANES + height, SUBLANES + height + 1))] = part[:1]


def get_plane(ref, at, height, offset=0):
    tiles = ref.shape[-3]
    first = SUBLANES + offset
    return jnp.concatenate([ref[(*at, tile, slice(first, first + height))] for tile in range(tiles)], axis=1)


def advance_plane(get, coeffs, row, time_step):
    centers, sums = [], []
    for field in (0, 1):
        center = get(field, row, 0)
        width = center.shape[1]
        total = get(field, row + 1, 0) + get(field, row - 1, 0)
        total = total + (get(field, row, -1) + get(field, row, 1))
        total = total + (pltpu.roll(center, 1, 1) + pltpu.roll(center, width - 1, 1))
        centers.append(center)
        sums.append(total)
    substrate, catalyst = centers
    reaction = (time_step * substrate) * (catalyst * catalyst)
    new_u = (coeffs(1, row) * substrate + spread_fast * sums[0]) + (coeffs(0, row) - reaction)
    new_v = (coeffs(2, row) * catalyst + spread_slow * sums[1]) + reaction
    return new_u, new_v


def pairing(shape, wide):
    pair = lax.broadcasted_iota(jnp.int32, shape, wide) // 2
    return jnp.where(pair == lax.broadcasted_iota(jnp.int32, shape, 1 - wide), 1.0, 0.0)


def restrict_planes(load, n_fields, rows, scratch):
    halves = []
    for field in range(n_fields):
        for pair in range(rows // 2):
            slot = field * (rows // 2) + pair
            plane = load(field, 2 * pair) + load(field, 2 * pair + 1)
            half = plane.shape[0] // 2
            lanes = []
            for at in range(plane.shape[1] // LANES):
                spot = slot * (plane.shape[1] // LANES) + at
                scratch[spot] = plane[:, at * LANES : (at + 1) * LANES]
                lanes.append(scratch[spot, pl.ds(0, half, 2), :] + scratch[spot, pl.ds(1, half, 2), :])
            halves.append(jnp.concatenate(lanes, axis=1))
    stacked = jnp.concatenate(halves, axis=0)
    width = stacked.shape[1]
    pool = pairing((width, width // 2), 0)
    pooled = jnp.dot(stacked, pool, precision=lax.Precision.HIGHEST, preferred_element_type=jnp.float32)
    return pooled * 0.125


def pack_call(arrays, places, outs, unit, moves, quartet=None, choice=None):
    scalars = [] if quartet is None else [quartet]

    def kernel(*refs):
        sources = refs[len(scalars) : len(scalars) + len(arrays)]
        results, sems = refs[len(scalars) + len(arrays) : -1], refs[-1]

        def move(at, source, target):
            return pltpu.make_async_copy(source, target, sems.at[at])

        copies = []
        for at, (array, index, out, slot, field) in enumerate(moves):
            source = sources[array] if index is None else sources[array].at[index]
            target = results[out].at[slot] if field is None else results[out].at[slot, field]
            copies.append(move(at, source, target))
        for copy in copies:
            copy.start()
        if choice is not None:
            there, special, (array, index), out = choice

            @pl.when(refs[0][0] == there)
            def _():
                copy = move(len(moves), sources[special], results[out].at[0])
                copy.start()
                copy.wait()

            @pl.when(refs[0][0] != there)
            def _():
                copy = move(len(moves), sources[array].at[index], results[out].at[0])
                copy.start()
                copy.wait()

        for copy in copies:
            copy.wait()

    specs = {"far": HBM, "near": VMEM}
    keep = {"far": far, "near": near}
    return pl.pallas_call(
        kernel,
        in_specs=[SMEM] * len(scalars) + [specs[p] for p in places],
        out_specs=[VMEM] * len(outs),
        out_shape=[pltpu.VMEM((n,) + unit, jnp.float32) for n in outs],
        scratch_shapes=[pltpu.SemaphoreType.DMA((len(moves) + 1,))],
        compiler_params=pltpu.CompilerParams(vmem_limit_bytes=VMEM_LIMIT),
    )(*scalars, *[keep[p](a) for p, a in zip(places, arrays)])


def first_call(parity, feed_rate, kill_rate, slice_ends, which):
    rows, sy, sz = feed_rate.shape
    reach = rows - 1

    def kernel(parity_ref, feed, kill, slices, units, planes, sems):
        near_rows = pl.ds(parity_ref[0], reach)
        moves = [
            (feed.at[near_rows], planes.at[pl.ds(2 * rows, reach)]),
            (kill.at[near_rows], planes.at[pl.ds(2 * rows + reach, reach)]),
            (slices.at[which, 0], planes.at[pl.ds(0, rows)]),
            (slices.at[which, 1], planes.at[pl.ds(rows, rows)]),
            (feed, units.at[0, 0]),
            (kill, units.at[0, 1]),
            (slices.at[which], units.at[1]),
        ]
        copies = [pltpu.make_async_copy(src, dst, sems.at[at]) for at, (src, dst) in enumerate(moves)]
        for copy in copies:
            copy.start()
        for copy in copies:
            copy.wait()

    return pl.pallas_call(
        kernel,
        in_specs=[SMEM] + [HBM] * 3,
        out_specs=[VMEM] * 2,
        out_shape=[
            pltpu.VMEM((2, 2, rows, sy, sz), jnp.float32),
            pltpu.VMEM((2 * rows + 2 * reach, sy, sz), jnp.float32),
        ],
        scratch_shapes=[pltpu.SemaphoreType.DMA((7,))],
        compiler_params=pltpu.CompilerParams(vmem_limit_bytes=VMEM_LIMIT),
        name="first",
    )(parity, far(feed_rate), far(kill_rate), far(slice_ends))


def gather_fine(odd, coeff_parts, buffers, plan, coef, ping):
    rows = coeff_parts[0].shape[2]

    def place(side, first, low=False):
        source, reach = coeff_parts[side], rows - 1
        if len(source.shape) == 3:
            for row in range(reach):
                feed, kill = source[2 * rows + row], source[2 * rows + reach + row]
                store_coeffs(coef, first + row + (1 if low else 0), feed, kill, fine_step)
        else:
            for row in range(rows):
                store_coeffs(coef, first + row, source[0, 0, row], source[0, 1, row], fine_step)
        for index, (at, slot) in enumerate(plan):
            part = buffers[at][side]
            for field in (0, 1):
                for row in range(rows):
                    plane = part[field * rows + row] if len(part.shape) == 3 else part[slot, field, row]
                    put_plane(ping, (index, field, first + row), plane)

    own, inner, outer = range(3)
    place(own, rows)

    @pl.when(odd == 0)
    def _():
        place(outer, 0, low=True)
        place(inner, 2 * rows)

    @pl.when(odd == 1)
    def _():
        place(inner, 0, low=True)
        place(outer, 2 * rows)


def advance_slice(index, rows, steps, coef, ping, pong, put):
    height, pair = coef.shape[-2], (ping, pong)
    for step in range(steps):
        src, dst = pair[step % 2], pair[(step + 1) % 2]
        first = rows - steps + 1 + step
        for row in range(first, 3 * rows - first):
            new = advance_plane(
                lambda field, r, offset: get_plane(src, (index, field, r), height, offset),
                lambda which, r: coef[which, r],
                row,
                fine_step,
            )
            for field in (0, 1):
                if step == steps - 1:
                    put(field, row - rows, new[field])
                else:
                    put_plane(dst, (index, field, row), new[field])


def fine_kernel(plan, rows, steps, n_buffers, bundled):
    def kernel(parity, *refs):
        refs = list(refs)
        coeff_parts = [refs.pop(0) for _ in range(3)]
        buffers = [tuple(refs.pop(0) for _ in range(3)) for _ in range(n_buffers)]
        rest = refs.pop(0) if bundled else None
        result = refs.pop(0)
        bundle = refs.pop(0) if bundled else None
        coef, ping, pong = refs[:3]
        gather_fine(parity[0], coeff_parts, buffers, plan, coef, ping)

        def one_slice(index, carry):
            def put(field, row, plane):
                result[index, field, row] = plane

            advance_slice(index, rows, steps, coef, ping, pong, put)
            return carry

        lax.fori_loop(0, len(plan), one_slice, 0)
        if bundled:
            pooled = restrict_planes(lambda f, r: result[0, f, r], 2, rows, refs[3])
            bundle[0:2] = pooled.reshape((2,) + bundle.shape[1:])
            bundle[2:] = rest[...]

    return kernel


def fine_call(parity, coeff_parts, buffers, plan, steps, rest=None):
    rows, sy, sz = coeff_parts[0].shape[-3:]
    n = len(plan)
    arrays = [*coeff_parts] + [part for buffer in buffers for part in buffer]
    scratch = [(3, 3 * rows, sy, sz)] + [padded_shape((n, 2, 3 * rows), sy, sz)] * 2
    outs = [(n, 2, rows, sy, sz)]
    if rest is not None:
        arrays.append(rest)
        outs.append((2 + rest.shape[0],) + rest.shape[1:])
        scratch.append((rows * sz // LANES, sy, LANES))
    kernel = fine_kernel(tuple(plan), rows, steps, len(buffers), rest is not None)
    return call(kernel, [parity], arrays, outs, scratch)


def early_kernel(rates, last, result, scratch):
    rows = rates.shape[2]

    def load(field, row):
        return last[0, field, row] if field < 2 else rates[0, field - 2, row]

    pooled = restrict_planes(load, 4, rows, scratch)
    result[...] = pooled.reshape(result.shape)


def early_call(last, rates):
    rows, sy, sz = rates.shape[-3:]
    shape = (4, rows // 2, sy // 2, sz // 2)
    return call(early_kernel, [], [rates, last], [shape], [(2 * rows * sz // LANES, sy, LANES)])[0]


def spread_blocks(odd, center, mine, theirs, put):
    depth = len(mine)

    @pl.when(odd == 0)
    def _():
        for at in range(depth):
            put(at, mine[at])
            put(2 * depth - at, theirs[at])

    @pl.when(odd == 1)
    def _():
        for at in range(depth):
            put(at, theirs[at])
            put(2 * depth - at, mine[at])

    put(depth, center)


def march(states, coef, base, middle, rows):
    height = coef.shape[-2]
    ends = [[[None] * rows, [None] * rows] for _ in states]
    for step in range(KC):
        reach = KC - 1 - step
        for row in range(middle - reach, middle + rows + reach):
            for pair, end in zip(states, ends):
                src, dst = pair[step % 2], pair[(step + 1) % 2]
                new = advance_plane(
                    lambda field, r, offset: get_plane(src, (field, base + r), height, offset),
                    lambda which, r: coef[which, base + r],
                    row,
                    coarse_step,
                )
                for field in (0, 1):
                    if step == KC - 1:
                        end[field][row - middle] = new[field]
                    else:
                        put_plane(dst, (field, base + row), new[field])
    return ends


def solve_first(depth, rows):
    def kernel(parity, *refs):
        center, mine, theirs = refs[0], refs[1 : 1 + depth], refs[1 + depth : 1 + 2 * depth]
        result, launch, coef, ping, pong, ping_l, pong_l = refs[1 + 2 * depth :]
        per = center.shape[1]

        def put(at, block):
            for r in range(per):
                row = at * per + r
                store_coeffs(coef, row, block[4, r], block[5, r], coarse_step)
                for field in (0, 1):
                    put_plane(ping, (field, row), block[field, r])
                    put_plane(ping_l, (field, row), block[2 + field, r])

        odd = parity[0]
        spread_blocks(odd, center, mine, theirs, put)
        base = rows * odd
        end, end_l = march([(ping, pong), (ping_l, pong_l)], coef, base, depth * per, rows)
        for field in (0, 1):
            for r in range(rows):
                launch[field, r] = end_l[field][r]
                result[field, r] = end[field][r] - end_l[field][r]

    return kernel


def solve_next(depth, rows):
    def kernel(parity, *refs):
        center, mine, theirs = refs[0], refs[1 : 1 + depth], refs[1 + depth : 1 + 2 * depth]
        launch, coef, result, ping, pong = refs[1 + 2 * depth :]
        per = center.shape[1]

        def put(at, block):
            for r in range(per):
                for field in (0, 1):
                    put_plane(ping, (field, at * per + r), block[field, r])

        odd = parity[0]
        spread_blocks(odd, center, mine, theirs, put)
        base = rows * odd
        (end,) = march([(ping, pong)], coef, base, depth * per, rows)
        for field in (0, 1):
            for r in range(rows):
                result[field, r] = end[field][r] - launch[field, r]

    return kernel


def solve_call(parity, blocks, rows, turns, known=None):
    center, mine, theirs = blocks
    _, per, sy, sz = center.shape
    total = ((2 * len(mine) + 1) * per, sy, sz)
    arrays = [center, *mine, *theirs]
    small, state = (2, rows, sy, sz), padded_shape((2, total[0]), sy, sz)
    if known is not None:
        kernel = solve_next(len(mine), rows)
        return call(kernel, [parity], [*arrays, *known], [small], [state] * 2)
    kernel, extra = solve_first(len(mine), rows), [small, (3,) + total]
    if turns > 1:
        return call(kernel, [parity], arrays, [small, *extra], [state] * 4)
    return call(kernel, [parity], arrays, [small], [*extra] + [state] * 4)


def final_call(parity, quartet, offset, coeff_parts, buffer, fines, steps, out_shape):
    rows, (sy, sz) = offset.shape[1], out_shape[-2:]
    last, earlier = CHUNKS[-1], CHUNKS[:-1]

    def kernel(parity_ref, quartet_ref, offset_ref, *refs):
        coeff_refs, buffer_refs, refs = refs[:3], refs[3:6], refs[6:]
        parts, refs = refs[: len(earlier)], refs[len(earlier) :]
        result, stage, shift, wide, coef, ping, pong, sems = refs
        first = quartet_ref[0] == 0
        planes = [offset_ref[f, r] for f in (0, 1) for r in range(rows)]
        stacked = jnp.concatenate(planes, axis=0)
        stacked = jnp.where(first, jnp.zeros_like(stacked), stacked)
        spread_out = jnp.dot(
            stacked, pairing((sz // 2, sz), 1), precision=lax.Precision.HIGHEST, preferred_element_type=jnp.float32
        )
        height, tiles = planes[0].shape[0], sz // LANES
        for i in range(len(planes)):
            part = spread_out[i * height : (i + 1) * height]
            for at in range(tiles):
                piece = part[:, at * LANES : (at + 1) * LANES]
                wide[i * tiles + at, pl.ds(0, height, 2), :] = piece
                wide[i * tiles + at, pl.ds(1, height, 2), :] = piece
            shift[i // rows, i % rows] = jnp.concatenate([wide[i * tiles + at] for at in range(tiles)], axis=1)
        copies = []

        def send(which):
            copies.append(pltpu.make_async_copy(stage.at[which], result.at[which], sems.at[which]))
            copies[-1].start()

        for chunk, part in zip(earlier, parts):
            for at, which in enumerate(chunk):
                for field in (0, 1):
                    for row in range(2 * rows):
                        stage[which, field, row] = part[at, field, row] + shift[field, row // 2]
                send(which)

        gather_fine(parity_ref[0], coeff_refs, [buffer_refs], [(0, k) for k in range(len(last))], coef, ping)
        for at, which in enumerate(last):

            def put(field, row, plane):
                stage[which, field, row] = plane + shift[field, row // 2]

            advance_slice(at, 2 * rows, steps, coef, ping, pong, put)
            send(which)
        for copy in copies:
            copy.wait()

    arrays = [offset, *coeff_parts, *buffer, *fines]
    slabs = padded_shape((len(last), 2, 6 * rows), sy, sz)
    return pl.pallas_call(
        kernel,
        in_specs=[SMEM] * 2 + [VMEM] * len(arrays),
        out_specs=ANY,
        out_shape=jax.ShapeDtypeStruct(out_shape, jnp.float32),
        scratch_shapes=[
            pltpu.VMEM(out_shape, jnp.float32),
            pltpu.VMEM((2, rows, sy, sz), jnp.float32),
            pltpu.VMEM((2 * rows * sz // LANES, sy, LANES), jnp.float32),
            pltpu.VMEM((3, 6 * rows, sy, sz), jnp.float32),
            pltpu.VMEM(slabs, jnp.float32),
            pltpu.VMEM(slabs, jnp.float32),
            pltpu.SemaphoreType.DMA((out_shape[0],)),
        ],
        compiler_params=pltpu.CompilerParams(vmem_limit_bytes=VMEM_LIMIT),
        name="final",
    )(parity, quartet, *[near(a) for a in arrays])


def whole_program(slice_ends, initial, feed_rate, kill_rate):
    rows = feed_rate.shape[0]
    count = slice_ends.shape[0]
    quartets = lax.axis_size("tm")
    size = lax.axis_size("space")
    tm = lax.axis_index("tm")
    odd = lax.axis_index("space") % 2
    parity, quartet = odd.astype(jnp.int32).reshape(1), tm.astype(jnp.int32).reshape(1)
    inner_pairs = [(i, i ^ 1) for i in range(size)]

    def across(value, reach):
        step = 2 * reach - 1
        pairs = [((i + step if i % 2 else i - step) % size, i) for i in range(size)]
        return lax.ppermute(value, "space", pairs)

    def swap(value):
        return lax.ppermute(value, "space", inner_pairs)

    def exchange(value, outward=None):
        outer = across(value if outward is None else outward, 1)
        return value, swap(value), outer

    def to_next(value, reach):
        step = 2 * reach - 1 if reach else 0
        pairs = []
        for t in range(quartets):
            for s in range(size):
                pairs.append((t * size + (s + step if s % 2 else s - step) % size, (t + 1) % quartets * size + s))
        return lax.ppermute(value, ("tm", "space"), pairs)

    coarse_rows = rows // 2
    depth = -(-KC // (2 * coarse_rows))

    def collect(value):
        other = swap(value)
        block = jnp.where(
            odd == 0, jnp.concatenate([value, other], axis=1), jnp.concatenate([other, value], axis=1)
        )
        mine = [to_next(block, depth - at) for at in range(depth)]
        center = to_next(block, 0)
        theirs = [swap(part) for part in mine]
        return center, mine, theirs

    width = min(rows, NF)
    assert width == rows and NF % width == 0 and size % 2 == 0
    rounds = NF // width

    unit = initial.shape
    first, outward = first_call(parity, feed_rate, kill_rate, slice_ends, CHUNKS[0][0] - 1)
    owns = [first]
    outs, moves = [len(chunk) for chunk in CHUNKS[1:-1]] + [1, 1], []
    for at, chunk in enumerate(CHUNKS[1:-1]):
        moves += [(0, i - 1, at, k, None) for k, i in enumerate(chunk)]
    moves.append((0, count - 1, len(outs) - 1, 0, None))
    *rest, sent, last = pack_call(
        [slice_ends, initial], ["far"] * 2, outs, unit, moves, quartet, (quartets - 1, 1, (0, count - 1), len(outs) - 2)
    )
    owns = [*owns, *rest]
    owns.append(to_next(sent, 0))
    buffers = [exchange(own, None if at else outward) for at, own in enumerate(owns)]
    coef_parts = buffers[0]
    rest = early_call(last, coef_parts[0])

    plans = [[(0, k + (1 if at == 0 else 0)) for k in range(len(chunk))] for at, chunk in enumerate(CHUNKS)]
    for turn in range(rounds):
        fines = []
        for at, chunk in enumerate(CHUNKS if turn < rounds - 1 else CHUNKS[:-1]):
            bundled = turn == rounds - 1 and at == 0
            got = fine_call(parity, coef_parts, [buffers[at]], plans[at], width, rest if bundled else None)
            fines.append(got[0])
            if bundled:
                bundle = got[1]
        if turn < rounds - 1:
            buffers = [exchange(fine) for fine in fines]
            plans = [[(0, k) for k in range(len(chunk))] for chunk in CHUNKS]

    blocks = collect(bundle)
    offset, *known = solve_call(parity, blocks, coarse_rows, quartets - 1)
    for _ in range(1, quartets - 1):
        guess = bundle[:2] + jnp.where(tm == 0, jnp.zeros_like(offset), offset)
        offset = solve_call(parity, collect(guess), coarse_rows, quartets - 1, known)[0]
    return final_call(
        parity, quartet, offset, coef_parts, buffers[-1], fines, width, slice_ends.shape
    )


def solution(mesh):
    in_specs = (
        P("tm", None, "space", None, None),
        P(None, "space", None, None),
        P("space", None, None),
        P("space", None, None),
    )
    out_specs = P("tm", None, "space", None, None)
    return jax.shard_map(whole_program, mesh=mesh, in_specs=in_specs, out_specs=out_specs, check_vma=False)
```

```python
import jax
import jax.numpy as jnp
import numpy as np
from jax import lax
from jax.experimental import pallas as pl
from jax.experimental.pallas import tpu as pltpu
from jax.sharding import PartitionSpec as P


NF = 8
KC = 8

spread_fast = 0.14
spread_slow = 0.07
fine_step = 0.25
coarse_step = 1.0

LANES = 128
VMEM_LIMIT = 12 << 20
CHUNKS = ((3,), (2, 1), (0,))

VMEM = pl.BlockSpec(memory_space=pltpu.VMEM)
SMEM = pl.BlockSpec(memory_space=pltpu.SMEM)
ANY = pl.BlockSpec(memory_space=pl.ANY)
HBM = pl.BlockSpec(memory_space=pltpu.HBM)


def near(value):
    return pltpu.with_memory_space_constraint(value, pltpu.VMEM)


def far(value):
    return pltpu.with_memory_space_constraint(value, pltpu.HBM)


def call(kernel, scalars, arrays, outs, scratch, far_out=False):
    shapes = [jax.ShapeDtypeStruct(o, jnp.float32) if far_out else pltpu.VMEM(o, jnp.float32) for o in outs]
    got = pl.pallas_call(
        kernel,
        in_specs=[SMEM] * len(scalars) + [VMEM] * len(arrays),
        out_specs=[VMEM] * len(outs),
        out_shape=shapes,
        scratch_shapes=[pltpu.VMEM(shape, jnp.float32) for shape in scratch],
        compiler_params=pltpu.CompilerParams(vmem_limit_bytes=VMEM_LIMIT),
    )(*scalars, *[near(a) for a in arrays])
    return got


def store_coeffs(coef, row, feed, kill, time_step):
    h_feed = time_step * feed
    coef[0, row] = h_feed
    coef[1, row] = (1.0 - 6.0 * spread_fast) - h_feed
    coef[2, row] = (1.0 - 6.0 * spread_slow) - (h_feed + time_step * kill)


def advance_plane(read, coeffs, row, time_step):
    centers, sums = [], []
    for field in (0, 1):
        center = read(field, row)
        height, width = center.shape
        total = read(field, row + 1) + read(field, row - 1)
        total = total + (pltpu.roll(center, 1, 0) + pltpu.roll(center, height - 1, 0))
        total = total + (pltpu.roll(center, 1, 1) + pltpu.roll(center, width - 1, 1))
        centers.append(center)
        sums.append(total)
    substrate, catalyst = centers
    reaction = (time_step * substrate) * (catalyst * catalyst)
    new_u = (coeffs(1, row) * substrate + spread_fast * sums[0]) + (coeffs(0, row) - reaction)
    new_v = (coeffs(2, row) * catalyst + spread_slow * sums[1]) + reaction
    return new_u, new_v


def pool_matrix(width):
    matrix = np.zeros((width, width // 2), np.float32)
    matrix[np.arange(width), np.arange(width) // 2] = 1.0
    return matrix


def restrict_planes(load, n_fields, rows, scratch, pool):
    halves = []
    for field in range(n_fields):
        for pair in range(rows // 2):
            slot = field * (rows // 2) + pair
            plane = load(field, 2 * pair) + load(field, 2 * pair + 1)
            half = plane.shape[0] // 2
            lanes = []
            for at in range(plane.shape[1] // LANES):
                spot = slot * (plane.shape[1] // LANES) + at
                scratch[spot] = plane[:, at * LANES : (at + 1) * LANES]
                lanes.append(scratch[spot, pl.ds(0, half, 2), :] + scratch[spot, pl.ds(1, half, 2), :])
            halves.append(jnp.concatenate(lanes, axis=1))
    stacked = jnp.concatenate(halves, axis=0)
    pooled = jnp.dot(stacked, pool, precision=lax.Precision.HIGHEST, preferred_element_type=jnp.float32)
    return pooled * 0.125


def pack_call(arrays, places, outs, unit, moves, quartet=None, choice=None):
    scalars = [] if quartet is None else [quartet]

    def kernel(*refs):
        sources = refs[len(scalars) : len(scalars) + len(arrays)]
        results, sems = refs[len(scalars) + len(arrays) : -1], refs[-1]

        def move(at, source, target):
            return pltpu.make_async_copy(source, target, sems.at[at])

        copies = []
        for at, (array, index, out, slot, field) in enumerate(moves):
            source = sources[array] if index is None else sources[array].at[index]
            target = results[out].at[slot] if field is None else results[out].at[slot, field]
            copies.append(move(at, source, target))
        for copy in copies:
            copy.start()
        if choice is not None:
            there, special, (array, index), out = choice

            @pl.when(refs[0][0] == there)
            def _():
                copy = move(len(moves), sources[special], results[out].at[0])
                copy.start()
                copy.wait()

            @pl.when(refs[0][0] != there)
            def _():
                copy = move(len(moves), sources[array].at[index], results[out].at[0])
                copy.start()
                copy.wait()

        for copy in copies:
            copy.wait()

    specs = {"far": HBM, "near": VMEM}
    keep = {"far": far, "near": near}
    return pl.pallas_call(
        kernel,
        in_specs=[SMEM] * len(scalars) + [specs[p] for p in places],
        out_specs=[VMEM] * len(outs),
        out_shape=[pltpu.VMEM((n,) + unit, jnp.float32) for n in outs],
        scratch_shapes=[pltpu.SemaphoreType.DMA((len(moves) + 1,))],
        compiler_params=pltpu.CompilerParams(vmem_limit_bytes=VMEM_LIMIT),
    )(*scalars, *[keep[p](a) for p, a in zip(places, arrays)])


def fine_kernel(plan, rows, steps, n_buffers, bundled):
    def kernel(parity, *refs):
        refs = list(refs)
        own_c, inn_c, out_c = [refs.pop(0) for _ in range(3)]
        buffers = [tuple(refs.pop(0) for _ in range(3)) for _ in range(n_buffers)]
        rest, pool = (refs.pop(0), refs.pop(0)) if bundled else (None, None)
        result = refs.pop(0)
        bundle = refs.pop(0) if bundled else None
        coef, ping, pong = refs[:3]
        odd = parity[0]

        def place_coef(source, at):
            for row in range(rows):
                store_coeffs(coef, at + row, source[0, 0, row], source[0, 1, row], fine_step)

        def place_halos(index, source, low, high):
            ping[index, :, 0:rows] = low[source]
            ping[index, :, 2 * rows : 3 * rows] = high[source]

        place_coef(own_c, rows)
        for index, (at, source) in enumerate(plan):
            ping[index, :, rows : 2 * rows] = buffers[at][0][source]

        @pl.when(odd == 0)
        def _():
            place_coef(out_c, 0)
            place_coef(inn_c, 2 * rows)
            for index, (at, source) in enumerate(plan):
                place_halos(index, source, buffers[at][2], buffers[at][1])

        @pl.when(odd == 1)
        def _():
            place_coef(inn_c, 0)
            place_coef(out_c, 2 * rows)
            for index, (at, source) in enumerate(plan):
                place_halos(index, source, buffers[at][1], buffers[at][2])

        def one_slice(index, carry):
            pair = (ping, pong)
            for step in range(steps):
                src, dst = pair[step % 2], pair[(step + 1) % 2]
                first = rows - steps + 1 + step
                for row in range(first, 3 * rows - first):
                    new = advance_plane(
                        lambda field, r: src[index, field, r], lambda which, r: coef[which, r], row, fine_step
                    )
                    for field in (0, 1):
                        if step == steps - 1:
                            result[index, field, row - rows] = new[field]
                        else:
                            dst[index, field, row] = new[field]
            return carry

        lax.fori_loop(0, len(plan), one_slice, 0)
        if bundled:
            pooled = restrict_planes(lambda f, r: result[0, f, r], 2, rows, refs[3], pool[...])
            bundle[0:2] = pooled.reshape((2,) + bundle.shape[1:])
            bundle[2:] = rest[...]

    return kernel


def fine_call(parity, coeff_parts, buffers, plan, steps, rest=None):
    rows, sy, sz = coeff_parts[0].shape[-3:]
    n = len(plan)
    arrays = [*coeff_parts] + [part for buffer in buffers for part in buffer]
    scratch = [(3, 3 * rows, sy, sz), (n, 2, 3 * rows, sy, sz), (n, 2, 3 * rows, sy, sz)]
    outs = [(n, 2, rows, sy, sz)]
    if rest is not None:
        arrays += [rest, jnp.asarray(pool_matrix(sz))]
        outs.append((2 + rest.shape[0],) + rest.shape[1:])
        scratch.append((rows * sz // LANES, sy, LANES))
    kernel = fine_kernel(tuple(plan), rows, steps, len(buffers), rest is not None)
    return call(kernel, [parity], arrays, outs, scratch)


def early_kernel(rates, last, pool, result, scratch):
    rows = rates.shape[2]

    def load(field, row):
        return last[0, field, row] if field < 2 else rates[0, field - 2, row]

    pooled = restrict_planes(load, 4, rows, scratch, pool[...])
    result[...] = pooled.reshape(result.shape)


def early_call(last, rates):
    rows, sy, sz = rates.shape[-3:]
    pool = jnp.asarray(pool_matrix(sz))
    shape = (4, rows // 2, sy // 2, sz // 2)
    return call(early_kernel, [], [rates, last, pool], [shape], [(2 * rows * sz // LANES, sy, LANES)])[0]


def spread_blocks(odd, center, mine, theirs, put):
    depth = len(mine)

    @pl.when(odd == 0)
    def _():
        for at in range(depth):
            put(at, mine[at])
            put(2 * depth - at, theirs[at])

    @pl.when(odd == 1)
    def _():
        for at in range(depth):
            put(at, theirs[at])
            put(2 * depth - at, mine[at])

    put(depth, center)


def march(state, coef, base, middle, rows):
    low = middle - KC
    planes = {(f, r): state[f, base + r] for f in (0, 1) for r in range(low, middle + rows + KC)}
    for step in range(KC):
        reach = KC - 1 - step
        new = {}
        for row in range(middle - reach, middle + rows + reach):
            pair = advance_plane(
                lambda field, r: planes[field, r], lambda which, r: coef[which, base + r], row, coarse_step
            )
            new[0, row], new[1, row] = pair
        planes = new
    return [[planes[f, middle + r] for r in range(rows)] for f in (0, 1)]


def solve_first(depth, rows):
    def kernel(parity, *refs):
        center, mine, theirs = refs[0], refs[1 : 1 + depth], refs[1 + depth : 1 + 2 * depth]
        result, launch, coef, ping, ping_l = refs[1 + 2 * depth :]
        per = center.shape[1]

        def put(at, block):
            for r in range(per):
                row = at * per + r
                store_coeffs(coef, row, block[4, r], block[5, r], coarse_step)
                for field in (0, 1):
                    ping[field, row] = block[field, r]
                    ping_l[field, row] = block[2 + field, r]

        odd = parity[0]
        spread_blocks(odd, center, mine, theirs, put)
        base = rows * odd
        end_l = march(ping_l, coef, base, depth * per, rows)
        end = march(ping, coef, base, depth * per, rows)
        for field in (0, 1):
            for r in range(rows):
                launch[field, r] = end_l[field][r]
                result[field, r] = end[field][r] - end_l[field][r]

    return kernel


def solve_next(depth, rows):
    def kernel(parity, *refs):
        center, mine, theirs = refs[0], refs[1 : 1 + depth], refs[1 + depth : 1 + 2 * depth]
        launch, coef, result, ping = refs[1 + 2 * depth :]
        per = center.shape[1]

        def put(at, block):
            for r in range(per):
                for field in (0, 1):
                    ping[field, at * per + r] = block[field, r]

        odd = parity[0]
        spread_blocks(odd, center, mine, theirs, put)
        base = rows * odd
        end = march(ping, coef, base, depth * per, rows)
        for field in (0, 1):
            for r in range(rows):
                result[field, r] = end[field][r] - launch[field, r]

    return kernel


def solve_call(parity, blocks, rows, known=None):
    center, mine, theirs = blocks
    _, per, sy, sz = center.shape
    total = ((2 * len(mine) + 1) * per, sy, sz)
    arrays = [center, *mine, *theirs]
    small, state = (2, rows, sy, sz), (2,) + total
    if known is None:
        return call(solve_first(len(mine), rows), [parity], arrays, [small, small, (3,) + total], [state] * 2)
    return call(solve_next(len(mine), rows), [parity], [*arrays, *known], [small], [state])


def final_call(quartet, offset, fines, out_shape):
    rows, (sy, sz) = offset.shape[1], out_shape[-2:]

    def kernel(quartet_ref, offset_ref, spread, *refs):
        parts, (result, stage, shift, wide, sems) = refs[: len(CHUNKS)], refs[len(CHUNKS) :]
        first = quartet_ref[0] == 0
        planes = [offset_ref[f, r] for f in (0, 1) for r in range(rows)]
        stacked = jnp.concatenate(planes, axis=0)
        stacked = jnp.where(first, jnp.zeros_like(stacked), stacked)
        spread_out = jnp.dot(
            stacked, spread[...], precision=lax.Precision.HIGHEST, preferred_element_type=jnp.float32
        )
        height, tiles = planes[0].shape[0], sz // LANES
        for i in range(len(planes)):
            part = spread_out[i * height : (i + 1) * height]
            for at in range(tiles):
                piece = part[:, at * LANES : (at + 1) * LANES]
                wide[i * tiles + at, pl.ds(0, height, 2), :] = piece
                wide[i * tiles + at, pl.ds(1, height, 2), :] = piece
            shift[i // rows, i % rows] = jnp.concatenate([wide[i * tiles + at] for at in range(tiles)], axis=1)
        copies = []
        for chunk, part in zip(CHUNKS, parts):
            for at, which in enumerate(chunk):
                for field in (0, 1):
                    for row in range(2 * rows):
                        stage[which, field, row] = part[at, field, row] + shift[field, row // 2]
                copies.append(pltpu.make_async_copy(stage.at[which], result.at[which], sems.at[which]))
                copies[-1].start()
        for copy in copies:
            copy.wait()

    arrays = [offset, jnp.asarray(pool_matrix(sz).T.copy()), *fines]
    return pl.pallas_call(
        kernel,
        in_specs=[SMEM] + [VMEM] * len(arrays),
        out_specs=ANY,
        out_shape=jax.ShapeDtypeStruct(out_shape, jnp.float32),
        scratch_shapes=[
            pltpu.VMEM(out_shape, jnp.float32),
            pltpu.VMEM((2, rows, sy, sz), jnp.float32),
            pltpu.VMEM((2 * rows * sz // LANES, sy, LANES), jnp.float32),
            pltpu.SemaphoreType.DMA((out_shape[0],)),
        ],
        compiler_params=pltpu.CompilerParams(vmem_limit_bytes=VMEM_LIMIT),
        name="final",
    )(quartet, *[near(a) for a in arrays])


def whole_program(slice_ends, initial, feed_rate, kill_rate):
    rows = feed_rate.shape[0]
    count = slice_ends.shape[0]
    quartets = lax.axis_size("tm")
    size = lax.axis_size("space")
    tm = lax.axis_index("tm")
    odd = lax.axis_index("space") % 2
    parity, quartet = odd.astype(jnp.int32).reshape(1), tm.astype(jnp.int32).reshape(1)
    inner_pairs = [(i, i ^ 1) for i in range(size)]

    def across(value, reach):
        step = 2 * reach - 1
        pairs = [((i + step if i % 2 else i - step) % size, i) for i in range(size)]
        return lax.ppermute(value, "space", pairs)

    def swap(value):
        return lax.ppermute(value, "space", inner_pairs)

    def exchange(value):
        outer = across(value, 1)
        return value, swap(value), outer

    def to_next(value, reach):
        step = 2 * reach - 1 if reach else 0
        pairs = []
        for t in range(quartets):
            for s in range(size):
                pairs.append((t * size + (s + step if s % 2 else s - step) % size, (t + 1) % quartets * size + s))
        return lax.ppermute(value, ("tm", "space"), pairs)

    coarse_rows = rows // 2
    depth = -(-KC // (2 * coarse_rows))

    def collect(value):
        other = swap(value)
        block = jnp.where(
            odd == 0, jnp.concatenate([value, other], axis=1), jnp.concatenate([other, value], axis=1)
        )
        mine = [to_next(block, depth - at) for at in range(depth)]
        center = to_next(block, 0)
        theirs = [swap(part) for part in mine]
        return center, mine, theirs

    width = min(rows, NF)
    assert width == rows and NF % width == 0 and size % 2 == 0
    rounds = NF // width

    unit = initial.shape
    moves = [(0, None, 0, 0, 0), (1, None, 0, 0, 1)] + [(2, i - 1, 0, k + 1, None) for k, i in enumerate(CHUNKS[0])]
    owns = pack_call([feed_rate, kill_rate, slice_ends], ["far"] * 3, [1 + len(CHUNKS[0])], unit, moves)
    outs, moves = [len(chunk) for chunk in CHUNKS[1:-1]] + [1, 1], []
    for at, chunk in enumerate(CHUNKS[1:-1]):
        moves += [(0, i - 1, at, k, None) for k, i in enumerate(chunk)]
    moves.append((0, count - 1, len(outs) - 1, 0, None))
    *rest, sent, last = pack_call(
        [slice_ends, initial], ["far"] * 2, outs, unit, moves, quartet, (quartets - 1, 1, (0, count - 1), len(outs) - 2)
    )
    owns = [*owns, *rest]
    owns.append(to_next(sent, 0))
    buffers = [exchange(own) for own in owns]
    coef_parts = buffers[0]
    rest = early_call(last, coef_parts[0])

    plans = [[(0, k + (1 if at == 0 else 0)) for k in range(len(chunk))] for at, chunk in enumerate(CHUNKS)]
    for turn in range(rounds):
        fines = []
        for at, chunk in enumerate(CHUNKS):
            bundled = turn == rounds - 1 and at == 0
            got = fine_call(parity, coef_parts, [buffers[at]], plans[at], width, rest if bundled else None)
            fines.append(got[0])
            if bundled:
                bundle = got[1]
        if turn < rounds - 1:
            buffers = [exchange(fine) for fine in fines]
            plans = [[(0, k) for k in range(len(chunk))] for chunk in CHUNKS]

    blocks = collect(bundle)
    offset, *known = solve_call(parity, blocks, coarse_rows)
    for _ in range(1, quartets - 1):
        guess = bundle[:2] + jnp.where(tm == 0, jnp.zeros_like(offset), offset)
        offset = solve_call(parity, collect(guess), coarse_rows, known)[0]
    return final_call(quartet, offset, fines, slice_ends.shape)


def solution(mesh):
    in_specs = (
        P("tm", None, "space", None, None),
        P(None, "space", None, None),
        P("space", None, None),
        P("space", None, None),
    )
    out_specs = P("tm", None, "space", None, None)
    return jax.shard_map(whole_program, mesh=mesh, in_specs=in_specs, out_specs=out_specs, check_vma=False)
```

```python
import jax
import jax.numpy as jnp
from jax import lax
from jax.experimental import pallas as pl
from jax.experimental.pallas import tpu as pltpu
from jax.sharding import PartitionSpec as P


NF = 8
KC = 8

spread_fast = 0.14
spread_slow = 0.07
fine_step = 0.25
coarse_step = 1.0

LANES = 128
SUBLANES = 8
VMEM_LIMIT = 12 << 20
CHUNKS = ((3,), (2, 1), (0,))

VMEM = pl.BlockSpec(memory_space=pltpu.VMEM)
SMEM = pl.BlockSpec(memory_space=pltpu.SMEM)
ANY = pl.BlockSpec(memory_space=pl.ANY)
HBM = pl.BlockSpec(memory_space=pltpu.HBM)


def near(value):
    return pltpu.with_memory_space_constraint(value, pltpu.VMEM)


def far(value):
    return pltpu.with_memory_space_constraint(value, pltpu.HBM)


def call(kernel, scalars, arrays, outs, scratch, far_out=False):
    shapes = [jax.ShapeDtypeStruct(o, jnp.float32) if far_out else pltpu.VMEM(o, jnp.float32) for o in outs]
    got = pl.pallas_call(
        kernel,
        in_specs=[SMEM] * len(scalars) + [VMEM] * len(arrays),
        out_specs=[VMEM] * len(outs),
        out_shape=shapes,
        scratch_shapes=[pltpu.VMEM(shape, jnp.float32) for shape in scratch],
        compiler_params=pltpu.CompilerParams(vmem_limit_bytes=VMEM_LIMIT),
    )(*scalars, *[near(a) for a in arrays])
    return got


def store_coeffs(coef, row, feed, kill, time_step):
    h_feed = time_step * feed
    coef[0, row] = h_feed
    coef[1, row] = (1.0 - 6.0 * spread_fast) - h_feed
    coef[2, row] = (1.0 - 6.0 * spread_slow) - (h_feed + time_step * kill)


def padded_shape(lead, sy, sz):
    return (*lead, sz // LANES, sy + 2 * SUBLANES, LANES)


def put_plane(ref, at, plane):
    height = plane.shape[0]
    for tile in range(plane.shape[1] // LANES):
        part = plane[:, tile * LANES : (tile + 1) * LANES]
        ref[(*at, tile, slice(SUBLANES, SUBLANES + height))] = part
        ref[(*at, tile, slice(SUBLANES - 1, SUBLANES))] = part[height - 1 :]
        ref[(*at, tile, slice(SUBLANES + height, SUBLANES + height + 1))] = part[:1]


def get_plane(ref, at, height, offset=0):
    tiles = ref.shape[-3]
    first = SUBLANES + offset
    return jnp.concatenate([ref[(*at, tile, slice(first, first + height))] for tile in range(tiles)], axis=1)


def advance_plane(get, coeffs, row, time_step):
    centers, sums = [], []
    for field in (0, 1):
        center = get(field, row, 0)
        width = center.shape[1]
        total = get(field, row + 1, 0) + get(field, row - 1, 0)
        total = total + (get(field, row, -1) + get(field, row, 1))
        total = total + (pltpu.roll(center, 1, 1) + pltpu.roll(center, width - 1, 1))
        centers.append(center)
        sums.append(total)
    substrate, catalyst = centers
    reaction = (time_step * substrate) * (catalyst * catalyst)
    new_u = (coeffs(1, row) * substrate + spread_fast * sums[0]) + (coeffs(0, row) - reaction)
    new_v = (coeffs(2, row) * catalyst + spread_slow * sums[1]) + reaction
    return new_u, new_v


def pairing(shape, wide):
    pair = lax.broadcasted_iota(jnp.int32, shape, wide) // 2
    return jnp.where(pair == lax.broadcasted_iota(jnp.int32, shape, 1 - wide), 1.0, 0.0)


def restrict_planes(load, n_fields, rows, scratch):
    halves = []
    for field in range(n_fields):
        for pair in range(rows // 2):
            slot = field * (rows // 2) + pair
            plane = load(field, 2 * pair) + load(field, 2 * pair + 1)
            half = plane.shape[0] // 2
            lanes = []
            for at in range(plane.shape[1] // LANES):
                spot = slot * (plane.shape[1] // LANES) + at
                scratch[spot] = plane[:, at * LANES : (at + 1) * LANES]
                lanes.append(scratch[spot, pl.ds(0, half, 2), :] + scratch[spot, pl.ds(1, half, 2), :])
            halves.append(jnp.concatenate(lanes, axis=1))
    stacked = jnp.concatenate(halves, axis=0)
    width = stacked.shape[1]
    pool = pairing((width, width // 2), 0)
    pooled = jnp.dot(stacked, pool, precision=lax.Precision.HIGHEST, preferred_element_type=jnp.float32)
    return pooled * 0.125


def pack_call(arrays, places, outs, unit, moves, quartet=None, choice=None):
    scalars = [] if quartet is None else [quartet]

    def kernel(*refs):
        sources = refs[len(scalars) : len(scalars) + len(arrays)]
        results, sems = refs[len(scalars) + len(arrays) : -1], refs[-1]

        def move(at, source, target):
            return pltpu.make_async_copy(source, target, sems.at[at])

        copies = []
        for at, (array, index, out, slot, field) in enumerate(moves):
            source = sources[array] if index is None else sources[array].at[index]
            target = results[out].at[slot] if field is None else results[out].at[slot, field]
            copies.append(move(at, source, target))
        for copy in copies:
            copy.start()
        if choice is not None:
            there, special, (array, index), out = choice

            @pl.when(refs[0][0] == there)
            def _():
                copy = move(len(moves), sources[special], results[out].at[0])
                copy.start()
                copy.wait()

            @pl.when(refs[0][0] != there)
            def _():
                copy = move(len(moves), sources[array].at[index], results[out].at[0])
                copy.start()
                copy.wait()

        for copy in copies:
            copy.wait()

    specs = {"far": HBM, "near": VMEM}
    keep = {"far": far, "near": near}
    return pl.pallas_call(
        kernel,
        in_specs=[SMEM] * len(scalars) + [specs[p] for p in places],
        out_specs=[VMEM] * len(outs),
        out_shape=[pltpu.VMEM((n,) + unit, jnp.float32) for n in outs],
        scratch_shapes=[pltpu.SemaphoreType.DMA((len(moves) + 1,))],
        compiler_params=pltpu.CompilerParams(vmem_limit_bytes=VMEM_LIMIT),
    )(*scalars, *[keep[p](a) for p, a in zip(places, arrays)])


def gather_fine(odd, coeff_parts, buffers, plan, coef, ping):
    rows = coeff_parts[0].shape[2]

    def place_coef(source, at):
        for row in range(rows):
            store_coeffs(coef, at + row, source[0, 0, row], source[0, 1, row], fine_step)

    def place(side, first):
        place_coef(coeff_parts[side], first)
        for index, (at, source) in enumerate(plan):
            for field in (0, 1):
                for row in range(rows):
                    put_plane(ping, (index, field, first + row), buffers[at][side][source, field, row])

    own, inner, outer = range(3)
    place(own, rows)

    @pl.when(odd == 0)
    def _():
        place(outer, 0)
        place(inner, 2 * rows)

    @pl.when(odd == 1)
    def _():
        place(inner, 0)
        place(outer, 2 * rows)


def advance_slice(index, rows, steps, coef, ping, pong, put):
    height, pair = coef.shape[-2], (ping, pong)
    for step in range(steps):
        src, dst = pair[step % 2], pair[(step + 1) % 2]
        first = rows - steps + 1 + step
        for row in range(first, 3 * rows - first):
            new = advance_plane(
                lambda field, r, offset: get_plane(src, (index, field, r), height, offset),
                lambda which, r: coef[which, r],
                row,
                fine_step,
            )
            for field in (0, 1):
                if step == steps - 1:
                    put(field, row - rows, new[field])
                else:
                    put_plane(dst, (index, field, row), new[field])


def fine_kernel(plan, rows, steps, n_buffers, bundled):
    def kernel(parity, *refs):
        refs = list(refs)
        coeff_parts = [refs.pop(0) for _ in range(3)]
        buffers = [tuple(refs.pop(0) for _ in range(3)) for _ in range(n_buffers)]
        rest = refs.pop(0) if bundled else None
        result = refs.pop(0)
        bundle = refs.pop(0) if bundled else None
        coef, ping, pong = refs[:3]
        gather_fine(parity[0], coeff_parts, buffers, plan, coef, ping)

        def one_slice(index, carry):
            def put(field, row, plane):
                result[index, field, row] = plane

            advance_slice(index, rows, steps, coef, ping, pong, put)
            return carry

        lax.fori_loop(0, len(plan), one_slice, 0)
        if bundled:
            pooled = restrict_planes(lambda f, r: result[0, f, r], 2, rows, refs[3])
            bundle[0:2] = pooled.reshape((2,) + bundle.shape[1:])
            bundle[2:] = rest[...]

    return kernel


def fine_call(parity, coeff_parts, buffers, plan, steps, rest=None):
    rows, sy, sz = coeff_parts[0].shape[-3:]
    n = len(plan)
    arrays = [*coeff_parts] + [part for buffer in buffers for part in buffer]
    scratch = [(3, 3 * rows, sy, sz)] + [padded_shape((n, 2, 3 * rows), sy, sz)] * 2
    outs = [(n, 2, rows, sy, sz)]
    if rest is not None:
        arrays.append(rest)
        outs.append((2 + rest.shape[0],) + rest.shape[1:])
        scratch.append((rows * sz // LANES, sy, LANES))
    kernel = fine_kernel(tuple(plan), rows, steps, len(buffers), rest is not None)
    return call(kernel, [parity], arrays, outs, scratch)


def early_kernel(rates, last, result, scratch):
    rows = rates.shape[2]

    def load(field, row):
        return last[0, field, row] if field < 2 else rates[0, field - 2, row]

    pooled = restrict_planes(load, 4, rows, scratch)
    result[...] = pooled.reshape(result.shape)


def early_call(last, rates):
    rows, sy, sz = rates.shape[-3:]
    shape = (4, rows // 2, sy // 2, sz // 2)
    return call(early_kernel, [], [rates, last], [shape], [(2 * rows * sz // LANES, sy, LANES)])[0]


def spread_blocks(odd, center, mine, theirs, put):
    depth = len(mine)

    @pl.when(odd == 0)
    def _():
        for at in range(depth):
            put(at, mine[at])
            put(2 * depth - at, theirs[at])

    @pl.when(odd == 1)
    def _():
        for at in range(depth):
            put(at, theirs[at])
            put(2 * depth - at, mine[at])

    put(depth, center)


def march(states, coef, base, middle, rows):
    height = coef.shape[-2]
    ends = [[[None] * rows, [None] * rows] for _ in states]
    for step in range(KC):
        reach = KC - 1 - step
        for row in range(middle - reach, middle + rows + reach):
            for pair, end in zip(states, ends):
                src, dst = pair[step % 2], pair[(step + 1) % 2]
                new = advance_plane(
                    lambda field, r, offset: get_plane(src, (field, base + r), height, offset),
                    lambda which, r: coef[which, base + r],
                    row,
                    coarse_step,
                )
                for field in (0, 1):
                    if step == KC - 1:
                        end[field][row - middle] = new[field]
                    else:
                        put_plane(dst, (field, base + row), new[field])
    return ends


def solve_first(depth, rows):
    def kernel(parity, *refs):
        center, mine, theirs = refs[0], refs[1 : 1 + depth], refs[1 + depth : 1 + 2 * depth]
        result, launch, coef, ping, pong, ping_l, pong_l = refs[1 + 2 * depth :]
        per = center.shape[1]

        def put(at, block):
            for r in range(per):
                row = at * per + r
                store_coeffs(coef, row, block[4, r], block[5, r], coarse_step)
                for field in (0, 1):
                    put_plane(ping, (field, row), block[field, r])
                    put_plane(ping_l, (field, row), block[2 + field, r])

        odd = parity[0]
        spread_blocks(odd, center, mine, theirs, put)
        base = rows * odd
        end, end_l = march([(ping, pong), (ping_l, pong_l)], coef, base, depth * per, rows)
        for field in (0, 1):
            for r in range(rows):
                launch[field, r] = end_l[field][r]
                result[field, r] = end[field][r] - end_l[field][r]

    return kernel


def solve_next(depth, rows):
    def kernel(parity, *refs):
        center, mine, theirs = refs[0], refs[1 : 1 + depth], refs[1 + depth : 1 + 2 * depth]
        launch, coef, result, ping, pong = refs[1 + 2 * depth :]
        per = center.shape[1]

        def put(at, block):
            for r in range(per):
                for field in (0, 1):
                    put_plane(ping, (field, at * per + r), block[field, r])

        odd = parity[0]
        spread_blocks(odd, center, mine, theirs, put)
        base = rows * odd
        (end,) = march([(ping, pong)], coef, base, depth * per, rows)
        for field in (0, 1):
            for r in range(rows):
                result[field, r] = end[field][r] - launch[field, r]

    return kernel


def solve_call(parity, blocks, rows, turns, known=None):
    center, mine, theirs = blocks
    _, per, sy, sz = center.shape
    total = ((2 * len(mine) + 1) * per, sy, sz)
    arrays = [center, *mine, *theirs]
    small, state = (2, rows, sy, sz), padded_shape((2, total[0]), sy, sz)
    if known is not None:
        kernel = solve_next(len(mine), rows)
        return call(kernel, [parity], [*arrays, *known], [small], [state] * 2)
    kernel, extra = solve_first(len(mine), rows), [small, (3,) + total]
    if turns > 1:
        return call(kernel, [parity], arrays, [small, *extra], [state] * 4)
    return call(kernel, [parity], arrays, [small], [*extra] + [state] * 4)


def final_call(parity, quartet, offset, coeff_parts, buffer, fines, steps, out_shape):
    rows, (sy, sz) = offset.shape[1], out_shape[-2:]
    last, earlier = CHUNKS[-1], CHUNKS[:-1]

    def kernel(parity_ref, quartet_ref, offset_ref, *refs):
        coeff_refs, buffer_refs, refs = refs[:3], refs[3:6], refs[6:]
        parts, refs = refs[: len(earlier)], refs[len(earlier) :]
        result, stage, shift, wide, coef, ping, pong, sems = refs
        first = quartet_ref[0] == 0
        planes = [offset_ref[f, r] for f in (0, 1) for r in range(rows)]
        stacked = jnp.concatenate(planes, axis=0)
        stacked = jnp.where(first, jnp.zeros_like(stacked), stacked)
        spread_out = jnp.dot(
            stacked, pairing((sz // 2, sz), 1), precision=lax.Precision.HIGHEST, preferred_element_type=jnp.float32
        )
        height, tiles = planes[0].shape[0], sz // LANES
        for i in range(len(planes)):
            part = spread_out[i * height : (i + 1) * height]
            for at in range(tiles):
                piece = part[:, at * LANES : (at + 1) * LANES]
                wide[i * tiles + at, pl.ds(0, height, 2), :] = piece
                wide[i * tiles + at, pl.ds(1, height, 2), :] = piece
            shift[i // rows, i % rows] = jnp.concatenate([wide[i * tiles + at] for at in range(tiles)], axis=1)
        copies = []

        def send(which):
            copies.append(pltpu.make_async_copy(stage.at[which], result.at[which], sems.at[which]))
            copies[-1].start()

        for chunk, part in zip(earlier, parts):
            for at, which in enumerate(chunk):
                for field in (0, 1):
                    for row in range(2 * rows):
                        stage[which, field, row] = part[at, field, row] + shift[field, row // 2]
                send(which)

        gather_fine(parity_ref[0], coeff_refs, [buffer_refs], [(0, k) for k in range(len(last))], coef, ping)
        for at, which in enumerate(last):

            def put(field, row, plane):
                stage[which, field, row] = plane + shift[field, row // 2]

            advance_slice(at, 2 * rows, steps, coef, ping, pong, put)
            send(which)
        for copy in copies:
            copy.wait()

    arrays = [offset, *coeff_parts, *buffer, *fines]
    slabs = padded_shape((len(last), 2, 6 * rows), sy, sz)
    return pl.pallas_call(
        kernel,
        in_specs=[SMEM] * 2 + [VMEM] * len(arrays),
        out_specs=ANY,
        out_shape=jax.ShapeDtypeStruct(out_shape, jnp.float32),
        scratch_shapes=[
            pltpu.VMEM(out_shape, jnp.float32),
            pltpu.VMEM((2, rows, sy, sz), jnp.float32),
            pltpu.VMEM((2 * rows * sz // LANES, sy, LANES), jnp.float32),
            pltpu.VMEM((3, 6 * rows, sy, sz), jnp.float32),
            pltpu.VMEM(slabs, jnp.float32),
            pltpu.VMEM(slabs, jnp.float32),
            pltpu.SemaphoreType.DMA((out_shape[0],)),
        ],
        compiler_params=pltpu.CompilerParams(vmem_limit_bytes=VMEM_LIMIT),
        name="final",
    )(parity, quartet, *[near(a) for a in arrays])


def whole_program(slice_ends, initial, feed_rate, kill_rate):
    rows = feed_rate.shape[0]
    count = slice_ends.shape[0]
    quartets = lax.axis_size("tm")
    size = lax.axis_size("space")
    tm = lax.axis_index("tm")
    odd = lax.axis_index("space") % 2
    parity, quartet = odd.astype(jnp.int32).reshape(1), tm.astype(jnp.int32).reshape(1)
    inner_pairs = [(i, i ^ 1) for i in range(size)]

    def across(value, reach):
        step = 2 * reach - 1
        pairs = [((i + step if i % 2 else i - step) % size, i) for i in range(size)]
        return lax.ppermute(value, "space", pairs)

    def swap(value):
        return lax.ppermute(value, "space", inner_pairs)

    def exchange(value):
        outer = across(value, 1)
        return value, swap(value), outer

    def to_next(value, reach):
        step = 2 * reach - 1 if reach else 0
        pairs = []
        for t in range(quartets):
            for s in range(size):
                pairs.append((t * size + (s + step if s % 2 else s - step) % size, (t + 1) % quartets * size + s))
        return lax.ppermute(value, ("tm", "space"), pairs)

    coarse_rows = rows // 2
    depth = -(-KC // (2 * coarse_rows))

    def collect(value):
        other = swap(value)
        block = jnp.where(
            odd == 0, jnp.concatenate([value, other], axis=1), jnp.concatenate([other, value], axis=1)
        )
        mine = [to_next(block, depth - at) for at in range(depth)]
        center = to_next(block, 0)
        theirs = [swap(part) for part in mine]
        return center, mine, theirs

    width = min(rows, NF)
    assert width == rows and NF % width == 0 and size % 2 == 0
    rounds = NF // width

    unit = initial.shape
    moves = [(0, None, 0, 0, 0), (1, None, 0, 0, 1)] + [(2, i - 1, 0, k + 1, None) for k, i in enumerate(CHUNKS[0])]
    owns = pack_call([feed_rate, kill_rate, slice_ends], ["far"] * 3, [1 + len(CHUNKS[0])], unit, moves)
    outs, moves = [len(chunk) for chunk in CHUNKS[1:-1]] + [1, 1], []
    for at, chunk in enumerate(CHUNKS[1:-1]):
        moves += [(0, i - 1, at, k, None) for k, i in enumerate(chunk)]
    moves.append((0, count - 1, len(outs) - 1, 0, None))
    *rest, sent, last = pack_call(
        [slice_ends, initial], ["far"] * 2, outs, unit, moves, quartet, (quartets - 1, 1, (0, count - 1), len(outs) - 2)
    )
    owns = [*owns, *rest]
    owns.append(to_next(sent, 0))
    buffers = [exchange(own) for own in owns]
    coef_parts = buffers[0]
    rest = early_call(last, coef_parts[0])

    plans = [[(0, k + (1 if at == 0 else 0)) for k in range(len(chunk))] for at, chunk in enumerate(CHUNKS)]
    for turn in range(rounds):
        fines = []
        for at, chunk in enumerate(CHUNKS if turn < rounds - 1 else CHUNKS[:-1]):
            bundled = turn == rounds - 1 and at == 0
            got = fine_call(parity, coef_parts, [buffers[at]], plans[at], width, rest if bundled else None)
            fines.append(got[0])
            if bundled:
                bundle = got[1]
        if turn < rounds - 1:
            buffers = [exchange(fine) for fine in fines]
            plans = [[(0, k) for k in range(len(chunk))] for chunk in CHUNKS]

    blocks = collect(bundle)
    offset, *known = solve_call(parity, blocks, coarse_rows, quartets - 1)
    for _ in range(1, quartets - 1):
        guess = bundle[:2] + jnp.where(tm == 0, jnp.zeros_like(offset), offset)
        offset = solve_call(parity, collect(guess), coarse_rows, quartets - 1, known)[0]
    return final_call(
        parity, quartet, offset, coef_parts, buffers[-1], fines, width, slice_ends.shape
    )


def solution(mesh):
    in_specs = (
        P("tm", None, "space", None, None),
        P(None, "space", None, None),
        P("space", None, None),
        P("space", None, None),
    )
    out_specs = P("tm", None, "space", None, None)
    return jax.shard_map(whole_program, mesh=mesh, in_specs=in_specs, out_specs=out_specs, check_vma=False)
```
